32 devices in a mesh: row: 8 (over y, x, core), col: 4 (over z).
Axes of the slice: x: 2, y: 2, z: 4, core: 2. Of those that a mesh axis runs over, the one named last changes fastest.
Arguments:
- slc_stack: float32 [20, 2, 64, 512], P(None, None, 'row', 'col'), may hold values from -6 to 6
- land_mask: int32 [64, 512], P('row', 'col'), may hold values from 0 to 1, as said below
Outputs:
- linked: float32 [20, 2, 64, 512], P(None, None, 'row', 'col')
- compressed_final: float32 [2, 64, 512], P(None, 'row', 'col')
- mean_strength: float32 [2], replicated
The draws below stay inside these ranges and needn't reach their ends.
Inputs may be any that keep to these rules, and one draw needn't show every extreme that they name: `land_mask`: 1 marks a valid pixel, 0 a water pixel.
All inputs are finite; a program needn't handle non-finite values.
Results may differ from the reference program's by a relative error of at most 0.00012.
Values sent between devices are 32-bit elements; how exact they have to be, the bound alone decides.
A program may use at most 64 MiB of HBM per device.

```python
import jax
import jax.numpy as jnp
import numpy as np
from jax import lax

M = 10
MS = 2
WIN = 11
ITERS = 4
CR = 8
NR = 64
NC = 512
DATES = 20


def draw_land_mask(key, part):
    tile_rows = NR // 16 + 2
    tile_cols = NC // 16 + 2
    offset_key, tile_key = jax.random.split(jax.random.fold_in(key, 11))
    offsets = jax.random.randint(offset_key, (2,), 0, 16)
    row_level = 33 + 67 * jnp.arange(tile_rows, dtype=jnp.int32) // (tile_rows - 1)
    col_level = 33 + 67 * jnp.arange(tile_cols, dtype=jnp.int32) // (tile_cols - 1)
    chance = row_level[:, None] * col_level[None, :]
    samples = jax.random.randint(tile_key, (tile_rows, tile_cols), 0, 10000)
    tiles = (samples < chance).astype(jnp.int32)
    row_tile = (jnp.arange(NR, dtype=jnp.int32) + offsets[0]) // 16
    col_tile = (jnp.arange(NC, dtype=jnp.int32) + offsets[1]) // 16
    return tiles[row_tile][:, col_tile]


def block_scale(stream_key, extent, cuts, smallest, largest):
    def one(position, blocks):
        draws = jax.random.uniform(jax.random.fold_in(jax.random.fold_in(stream_key, 6), position), (blocks,), jnp.float32, smallest / len(cuts), largest / len(cuts))
        return jnp.repeat(jnp.exp(draws), extent[position] // blocks).reshape((-1,) + (1,) * (len(extent) - position - 1))

    loudness = one(*cuts[0])
    for cut in cuts[1:]:
        loudness = loudness * one(*cut)
    return loudness


def gaussian(own_key, dims, scale, most, cuts=(), held_as=jnp.bfloat16):
    values = jax.random.normal(own_key, dims, jnp.float32) * scale
    if len(cuts) > 0:
        values = block_scale(own_key, dims, cuts, -0.22, 0.18) * values
    return jnp.clip(values, min=-most, max=most).astype(held_as)


def setup_inputs(seed: int = 0) -> dict:
    streams_of = jax.random.split(jax.random.key(seed), 3)
    slc_stack = gaussian(streams_of[0], (DATES, 2, NR, NC), 1.0, 6.0, ((2, 8), (3, 4)), jnp.float32)
    land_mask = draw_land_mask(jax.random.fold_in(streams_of[2], 71), 0)
    return dict(slc_stack=slc_stack, land_mask=land_mask)


covariance_floor = 8.0

def pair_tables(number):
    upper_first, upper_second = np.triu_indices(number)
    strict_first, strict_second = np.triu_indices(number, 1)
    real_slot = np.zeros((number, number), np.int32)
    real_slot[upper_first, upper_second] = np.arange(upper_first.size)
    real_slot[upper_second, upper_first] = np.arange(upper_first.size)
    base_slot = upper_first.size
    imag_slot = np.full((number, number), base_slot + strict_first.size, np.int32)
    imag_sign = np.zeros((number, number), np.float32)
    imag_slot[strict_first, strict_second] = base_slot + np.arange(strict_first.size)
    imag_slot[strict_second, strict_first] = base_slot + np.arange(strict_first.size)
    imag_sign[strict_first, strict_second] = 1.0
    imag_sign[strict_second, strict_first] = -1.0
    return (upper_first, upper_second, strict_first, strict_second, real_slot.reshape(-1), imag_slot.reshape(-1), imag_sign.reshape(-1))

def pair_products(padded, tables):
    upper_first, upper_second, strict_first, strict_second = (tables[0], tables[1], tables[2], tables[3])
    left_upper = padded[upper_first]
    right_upper = padded[upper_second]
    real_fields = left_upper[:, 0] * right_upper[:, 0] + left_upper[:, 1] * right_upper[:, 1]
    left_strict = padded[strict_first]
    right_strict = padded[strict_second]
    imag_fields = left_strict[:, 1] * right_strict[:, 0] - left_strict[:, 0] * right_strict[:, 1]
    return jnp.concatenate([real_fields, imag_fields], 0)

def box_sum(products, height, width, reach):
    along_rows = products[:, 0:height, :]
    for offset in range(1, 2 * reach + 1):
        along_rows = along_rows + products[:, offset:offset + height, :]
    windowed = along_rows[:, :, 0:width]
    for offset in range(1, 2 * reach + 1):
        windowed = windowed + along_rows[:, :, offset:offset + width]
    return windowed

def finish(windowed, fresh, land_float, number, tables):
    real_slot, imag_slot, imag_sign = (tables[4], tables[5], tables[6])
    shape_tail = windowed.shape[1:]
    extended = jnp.concatenate([windowed, jnp.zeros_like(windowed[:1])], 0)
    cov_real = windowed[real_slot].reshape((number, number) + shape_tail)
    cov_imag = (extended[imag_slot] * imag_sign[:, None, None]).reshape((number, number) + shape_tail)
    diagonal = windowed[real_slot[::number + 1]]
    scales = 1.0 / jnp.sqrt(jnp.maximum(diagonal, covariance_floor))
    coh_real = cov_real * scales[:, None] * scales[None, :]
    coh_imag = cov_imag * scales[:, None] * scales[None, :]
    vec_real = jnp.ones((number,) + shape_tail, jnp.float32)
    vec_imag = jnp.zeros((number,) + shape_tail, jnp.float32)
    length = jnp.zeros(shape_tail, jnp.float32)
    for iteration in range(ITERS):
        next_real = lax.optimization_barrier(jnp.sum(coh_real * vec_real[None] - coh_imag * vec_imag[None], axis=1))
        next_imag = lax.optimization_barrier(jnp.sum(coh_real * vec_imag[None] + coh_imag * vec_real[None], axis=1))
        length = jnp.sqrt(lax.optimization_barrier(jnp.sum(next_real * next_real + next_imag * next_imag, axis=0)))
        divisor = jnp.maximum(length, 1.0)
        vec_real = next_real / divisor
        vec_imag = next_imag / divisor
    strength = jnp.sum(land_float * length) / number
    new_real = vec_real[number - M:]
    new_imag = vec_imag[number - M:]
    comp_real = lax.optimization_barrier(jnp.sum(new_real * fresh[:, 0] + new_imag * fresh[:, 1], axis=0))
    comp_imag = lax.optimization_barrier(jnp.sum(new_real * fresh[:, 1] - new_imag * fresh[:, 0], axis=0))
    linked_part = jnp.stack([new_real, new_imag], 1) * land_float
    compressed = jnp.stack([comp_real, comp_imag], 0)[None]
    return (linked_part, compressed, strength)

def reference(slc_stack, land_mask):
    reach = WIN // 2
    land_float = land_mask.astype(jnp.float32)
    signal = slc_stack * land_float
    strip_count = NR // CR
    carried_list = []
    linked_parts = []
    totals = []
    compressed = None
    for ministack in range(MS):
        number = ministack + M
        tables = pair_tables(number)
        fresh = signal[ministack * M:(ministack + 1) * M]
        stacked = jnp.concatenate(carried_list + [fresh], 0)
        padded = jnp.pad(stacked, ((0, 0), (0, 0), (reach, reach), (reach, reach)))

        def strip_work(strip_index, padded=padded, fresh=fresh, number=number, tables=tables):
            top = strip_index * CR
            block = lax.dynamic_slice_in_dim(padded, top, CR + 2 * reach, 2)
            fresh_block = lax.dynamic_slice_in_dim(fresh, top, CR, 2)
            land_block = lax.dynamic_slice_in_dim(land_float, top, CR, 0)
            products = pair_products(block, tables)
            windowed = box_sum(products, CR, NC, reach)
            return finish(windowed, fresh_block, land_block, number, tables)
        linked_strips, comp_strips, strength_strips = lax.map(strip_work, jnp.arange(strip_count, dtype=jnp.int32))
        linked_parts.append(jnp.transpose(linked_strips, (1, 2, 0, 3, 4)).reshape(M, 2, NR, NC))
        compressed = jnp.transpose(comp_strips, (1, 2, 0, 3, 4)).reshape(1, 2, NR, NC)
        carried_list.append(compressed)
        totals.append(jnp.sum(strength_strips))
    mean_strength = jnp.stack(totals) / (NR * NC)
    return (jnp.concatenate(linked_parts, 0), compressed[0], mean_strength)
```

```python
import functools

import jax
import jax.numpy as jnp
from jax import lax
from jax.experimental import pallas as pl
from jax.experimental.pallas import tpu as pltpu
from jax.sharding import PartitionSpec as P

M = 10
MS = 2
WIN = 11
ITERS = 4
REACH = WIN // 2
SUB = 8

covariance_floor = 8.0

AROUND = ((-1, 0), (1, 0), (-1, -1), (0, -1), (1, -1), (-1, 1), (0, 1), (1, 1))
SLOTS = M + SUB
HALO_ROWS = 24
HALO_ROOM = 40


def fresh_units():
    units = [((0, 0, 0), (SUB, 0, 0))]
    for lag in range(1, M):
        for first in range(0, M - lag, SUB):
            units.append(((first, lag, 0), (first, lag, 1)))
    return units


def field_of(units):
    table = {}
    for index, unit in enumerate(units):
        for half, (first, lag, part) in enumerate(unit):
            for lane in range(SUB):
                i = first + lane
                if i + lag < M:
                    table[(i, i + lag, part)] = index * 2 * SUB + half * SUB + lane
    return table


FRESH = fresh_units()
FIELDS = field_of(FRESH)


def window_sums(lines, outputs):
    core = lines[outputs - 1]
    for e in range(outputs, WIN):
        core = core + lines[e]
    low = [None] * outputs
    low[outputs - 1] = core
    for r in range(outputs - 2, -1, -1):
        low[r] = low[r + 1] + lines[r]
    sums = [low[0]]
    high = None
    for r in range(1, outputs):
        extra = lines[WIN - 1 + r]
        high = extra if high is None else high + extra
        sums.append(low[r] + high)
    return sums


def split(value):
    high = value.astype(jnp.bfloat16)
    low = (value - high.astype(jnp.float32)).astype(jnp.bfloat16)
    return high, low


def kernel(
    row_count,
    col_count,
    slc,
    land,
    linked,
    comp_out,
    strength,
    sig,
    up,
    dn,
    pack_send,
    pack_recv,
    halo,
    comp_send,
    comp_up,
    comp_dn,
    cpack_send,
    cpack_recv,
    w_main,
    w_halo,
    ybuf,
    hbuf,
    zbuf,
    ycbuf,
    hcbuf,
    zcbuf,
    coh,
    part,
    red_row,
    red_col,
    send_a,
    recv_a,
    send_b,
    recv_b,
    send_r,
    recv_r,
    send_c,
    recv_c,
):
    rows, cols = land.shape
    my_row = lax.axis_index("row")
    my_col = lax.axis_index("col")
    strip = rows * REACH

    exists = []
    for dr, dc in AROUND:
        ok = None
        for pos, step, count in ((my_row, dr, row_count), (my_col, dc, col_count)):
            if step:
                here = (pos > 0) if step < 0 else (pos < count - 1)
                ok = here if ok is None else jnp.logical_and(ok, here)
        exists.append(ok)

    for k, (dr, dc) in enumerate(AROUND):

        @pl.when(jnp.logical_not(exists[k]))
        def _(k=k, dc=dc, dr=dr):
            if dc == 0:
                target, small = (up, comp_up) if dr < 0 else (dn, comp_dn)
                for m in range(MS):
                    target[m] = jnp.zeros(target.shape[1:], jnp.float32)
                small[...] = jnp.zeros_like(small)
            else:
                for m in range(MS):
                    pack_recv[m, k - 2] = jnp.zeros(pack_recv.shape[2:], jnp.float32)
                cpack_recv[k - 2] = jnp.zeros(cpack_recv.shape[1:], jnp.float32)

    barrier = pltpu.get_barrier_semaphore()
    mesh_id = pl.DeviceIdType.MESH
    expected = jnp.int32(row_count - 1 + col_count - 1)
    for step in range(1, row_count):
        pl.semaphore_signal(
            barrier, inc=1, device_id=(lax.rem(my_row + step, row_count), my_col), device_id_type=mesh_id
        )
    for step in range(1, col_count):
        pl.semaphore_signal(
            barrier, inc=1, device_id=(my_row, lax.rem(my_col + step, col_count)), device_id_type=mesh_id
        )
    for k, (dr, dc) in enumerate(AROUND):
        if dr and dc:

            @pl.when(exists[k])
            def _(dr=dr, dc=dc):
                pl.semaphore_signal(
                    barrier, inc=1, device_id=(my_row + dr, my_col + dc), device_id_type=mesh_id
                )

            expected = expected + exists[k].astype(jnp.int32)

    mask = land[...].astype(jnp.float32)
    for m in range(MS):
        for i in range(M):
            for c in range(2):
                at = (i * 2 + c) * rows
                sig[m, at : at + rows, :] = slc[m * M + i, c] * mask
        for buffer in (sig, up, dn):
            buffer[m, M * 2 * rows :, :] = jnp.zeros((buffer.shape[1] - M * 2 * rows, cols), jnp.float32)

    lane = lax.broadcasted_iota(jnp.int32, (rows, cols), 1)
    sub = lax.broadcasted_iota(jnp.int32, (rows, cols), 0)
    from_right = (lane >= sub * REACH) & (lane < sub * REACH + REACH)
    from_left = (lane >= (sub + 1) * REACH) & (lane < (sub + 2) * REACH)

    def pack_tile(tile):
        turned = pltpu.roll(tile, REACH, 1, stride=REACH, stride_axis=0)
        high = jnp.sum(jnp.where(from_right, turned, 0.0), axis=0, keepdims=True)
        low = jnp.sum(jnp.where(from_left, turned, 0.0), axis=0, keepdims=True)
        return low, high

    def spread(line, shift):
        total = pltpu.roll(line, cols - shift, 1) if shift else line
        return (
            total
            + pltpu.roll(line, (strip - shift) % cols, 1)
            + pltpu.roll(line, (2 * strip - shift) % cols, 1)
        )

    for m in range(MS):
        pack_send[m] = jnp.zeros(pack_send.shape[1:], jnp.float32)
        for i in range(M):
            for c in range(2):
                low, high = pack_tile(sig[m, (i * 2 + c) * rows : (i * 2 + c + 1) * rows, :])
                pack_send[m, 0, c * (M + 1) + i : c * (M + 1) + i + 1, :] = low
                pack_send[m, 1, c * (M + 1) + i : c * (M + 1) + i + 1, :] = high
        pack_send[m, 0] = spread(pack_send[m, 0], REACH)
        pack_send[m, 1] = spread(pack_send[m, 1], 0)
        pack_recv[m, :, HALO_ROWS:, :] = jnp.zeros((6, HALO_ROOM - HALO_ROWS, cols), jnp.float32)

    pl.semaphore_wait(barrier, expected)

    def mirror(k):
        dr, dc = AROUND[k]
        return AROUND.index((-dr, -dc))

    def fresh_copy(m, k):
        dr, dc = AROUND[k]
        back = mirror(k)
        if dc == 0:
            source = sig.at[m, pl.ds(0, M * 2 * rows)]
            target = (dn if dr < 0 else up).at[m, pl.ds(0, M * 2 * rows)]
        else:
            source = pack_send.at[m, 0 if dc < 0 else 1]
            target = pack_recv.at[m, back - 2, pl.ds(0, HALO_ROWS)]
        return pltpu.make_async_remote_copy(
            src_ref=source,
            dst_ref=target,
            send_sem=send_a.at[m, k],
            recv_sem=recv_a.at[m, back],
            device_id=(my_row + dr, my_col + dc),
            device_id_type=mesh_id,
        )

    def fresh_arrival(m, k):
        dr, dc = AROUND[k]
        if dc == 0:
            source = sig.at[m, pl.ds(0, M * 2 * rows)]
            target = (up if dr < 0 else dn).at[m, pl.ds(0, M * 2 * rows)]
        else:
            source = pack_send.at[m, 0 if dc < 0 else 1]
            target = pack_recv.at[m, k - 2, pl.ds(0, HALO_ROWS)]
        return pltpu.make_async_remote_copy(
            src_ref=source,
            dst_ref=target,
            send_sem=send_a.at[m, k],
            recv_sem=recv_a.at[m, k],
            device_id=(my_row + dr, my_col + dc),
            device_id_type=mesh_id,
        )

    def each_around(action):
        for k in range(len(AROUND)):

            @pl.when(exists[k])
            def _(k=k):
                action(k)

    for m in range(MS):
        each_around(lambda k, m=m: fresh_copy(m, k).start())

    k_at = lax.broadcasted_iota(jnp.int32, (cols, cols), 0)
    n_at = lax.broadcasted_iota(jnp.int32, (cols, cols), 1)
    near = jnp.where((k_at - n_at <= REACH) & (n_at - k_at <= REACH), 1.0, 0.0).astype(jnp.bfloat16)
    w_main[0:cols, :] = near
    w_main[cols:, :] = near
    line_of = k_at // REACH
    inner = k_at - line_of * REACH
    for side in range(2):
        touches = (n_at <= inner) if side == 0 else (n_at >= inner + cols - REACH)
        line = jnp.where(touches, line_of, -1)
        for r in range(rows):
            first = rows - REACH + r
            w_halo[side * cols : (side + 1) * cols, r * cols : (r + 1) * cols] = jnp.where(
                (line >= first) & (line < first + WIN), 1.0, 0.0
            ).astype(jnp.bfloat16)

    outer = (up, sig, dn)
    lane_halo = lax.broadcasted_iota(jnp.int32, (HALO_ROOM, cols), 1)

    def gather_halo(m, parts, target):
        for side in range(2):
            a, b, c = (parts(side * 3 + j) for j in range(3))
            which = lane_halo[: a.shape[0]]
            target(side, jnp.where(which < strip, a, jnp.where(which < 2 * strip, b, c)))

    def line_tile(m, e, c, first):
        at = rows - REACH + e
        buffer = outer[at // rows]
        return buffer[m, pl.ds((first * 2 + c) * rows + at % rows, SUB, stride=2 * rows), :]

    def halo_tile(m, side, c, first):
        at = c * (M + 1) + first
        return halo[m, side, at : at + SUB, :]

    def emit(index, halves, ytarget, htarget):
        lines_total = WIN + rows - 1
        both = [jnp.concatenate([x, y], 0) for x, y in zip(halves[0], halves[1])]
        at = slice(index * 2 * SUB, (index + 1) * 2 * SUB)
        for r, total in enumerate(window_sums(both[:lines_total], rows)):
            high, low = split(total)
            ytarget[r, at, 0:cols] = high
            ytarget[r, at, cols:] = low
        for side in range(2):
            high, low = split(both[lines_total + side])
            htarget[0, at, side * cols : (side + 1) * cols] = high
            htarget[1, at, side * cols : (side + 1) * cols] = low

    def sources(m):
        lines_total = WIN + rows - 1
        return [functools.partial(line_tile, m, e) for e in range(lines_total)] + [
            functools.partial(halo_tile, m, side) for side in range(2)
        ]

    def real_part(a, b, x, y):
        return a * x + b * y

    def imag_part(a, b, x, y):
        return b * x - a * y

    def fresh_fields(m):
        for index, unit in enumerate(FRESH):
            halves = ([], [])
            for tile in sources(m):
                if index == 0:
                    for half in range(2):
                        first = unit[half][0]
                        a, b = tile(0, first), tile(1, first)
                        halves[half].append(a * a + b * b)
                else:
                    first, lag, _ = unit[0]
                    a, b = tile(0, first), tile(1, first)
                    x, y = tile(0, first + lag), tile(1, first + lag)
                    halves[0].append(real_part(a, b, x, y))
                    halves[1].append(imag_part(a, b, x, y))
            emit(index, halves, ybuf, hbuf)

    def windowed(ysource, hsource, target):
        count = ysource.shape[1]
        main = jnp.dot(
            ysource[...].reshape(rows * count, 2 * cols), w_main[...], preferred_element_type=jnp.float32
        )
        for r in range(rows):
            band = w_halo[:, r * cols : (r + 1) * cols]
            edge = jnp.dot(hsource[0], band, preferred_element_type=jnp.float32) + jnp.dot(
                hsource[1], band, preferred_element_type=jnp.float32
            )
            target[r * count : (r + 1) * count, :] = main[r * count : (r + 1) * count, :] + edge

    fresh_count = len(FRESH) * 2 * SUB

    def fresh_field(i, j, p):
        return zbuf[pl.ds(FIELDS[(i, j, p)], rows, stride=fresh_count), :]

    def power(number, field):
        scales = [
            lax.rsqrt(jnp.maximum(field(i, i, 0), covariance_floor)) for i in range(number)
        ]
        vec_re = [None] * number
        vec_im = [None] * number

        def add(store, i, value):
            store[i] = value if store[i] is None else store[i] + value

        def sub_(store, i, value):
            store[i] = -value if store[i] is None else store[i] - value

        slot = {}
        next_slot = 0
        for i in range(number):
            c = field(i, i, 0) * (scales[i] * scales[i])
            coh[next_slot] = c
            slot[(i, i, 0)] = next_slot
            next_slot += 1
            add(vec_re, i, c)
            for j in range(i + 1, number):
                s = scales[i] * scales[j]
                c = field(i, j, 0) * s
                d = field(i, j, 1) * s
                coh[next_slot] = c
                coh[next_slot + 1] = d
                slot[(i, j, 0)] = next_slot
                slot[(i, j, 1)] = next_slot + 1
                next_slot += 2
                add(vec_re, i, c)
                add(vec_re, j, c)
                add(vec_im, i, d)
                sub_(vec_im, j, d)

        def normalise():
            squares = None
            for i in range(number):
                both = vec_re[i] * vec_re[i] + vec_im[i] * vec_im[i]
                squares = both if squares is None else squares + both
            length = jnp.sqrt(squares)
            inverse = 1.0 / jnp.maximum(length, 1.0)
            return length, [v * inverse for v in vec_re], [v * inverse for v in vec_im]

        length, old_re, old_im = normalise()
        for _ in range(1, ITERS):
            vec_re = [None] * number
            vec_im = [None] * number
            for i in range(number):
                c = coh[slot[(i, i, 0)]]
                add(vec_re, i, c * old_re[i])
                add(vec_im, i, c * old_im[i])
                for j in range(i + 1, number):
                    c = coh[slot[(i, j, 0)]]
                    d = coh[slot[(i, j, 1)]]
                    add(vec_re, i, c * old_re[j] - d * old_im[j])
                    add(vec_im, i, c * old_im[j] + d * old_re[j])
                    add(vec_re, j, c * old_re[i] + d * old_im[i])
                    add(vec_im, j, c * old_im[i] - d * old_re[i])
            length, old_re, old_im = normalise()
        return length, old_re, old_im

    def finish(m, number, field):
        length, re, im = power(number, field)
        re, im = re[number - M :], im[number - M :]
        comp_re = comp_im = None
        for i in range(M):
            a = sig[m, i * 2 * rows : (i * 2 + 1) * rows, :]
            b = sig[m, (i * 2 + 1) * rows : (i * 2 + 2) * rows, :]
            x = re[i] * a + im[i] * b
            y = re[i] * b - im[i] * a
            comp_re = x if comp_re is None else comp_re + x
            comp_im = y if comp_im is None else comp_im + y
            linked[m * M + i, 0] = re[i] * mask
            linked[m * M + i, 1] = im[i] * mask
        part[m : m + 1, :] = jnp.sum(mask * length, axis=0, keepdims=True) * (1.0 / number)
        return comp_re, comp_im

    def take_fresh(m):
        each_around(lambda k: fresh_arrival(m, k).wait_recv())

        def put(side, value):
            halo[m, side] = value

        gather_halo(m, lambda j: pack_recv[m, j], put)

    take_fresh(0)
    fresh_fields(0)
    windowed(ybuf, hbuf, zbuf)
    comp_re, comp_im = finish(0, M, fresh_field)
    comp_send[0:rows, :] = comp_re
    comp_send[rows:, :] = comp_im
    cpack_send[...] = jnp.zeros_like(cpack_send)
    for c, value in enumerate((comp_re, comp_im)):
        low, high = pack_tile(value)
        cpack_send[0, c : c + 1, :] = spread(low, REACH)
        cpack_send[1, c : c + 1, :] = spread(high, 0)

    def comp_pair(k, sending):
        dr, dc = AROUND[k]
        slot = mirror(k) if sending else k
        if dc == 0:
            source = comp_send
            target = comp_up if AROUND[slot][0] < 0 else comp_dn
        else:
            source = cpack_send.at[0 if dc < 0 else 1]
            target = cpack_recv.at[slot - 2]
        return pltpu.make_async_remote_copy(
            src_ref=source,
            dst_ref=target,
            send_sem=send_b.at[k],
            recv_sem=recv_b.at[slot],
            device_id=(my_row + dr, my_col + dc),
            device_id_type=mesh_id,
        )

    each_around(lambda k: comp_pair(k, True).start())

    last = MS - 1
    take_fresh(last)
    fresh_fields(last)
    windowed(ybuf, hbuf, zbuf)

    each_around(lambda k: comp_pair(k, False).wait_recv())
    at = M * 2 * rows
    sig[last, at : at + 2 * rows, :] = comp_send[...]
    up[last, at : at + 2 * rows, :] = comp_up[...]
    dn[last, at : at + 2 * rows, :] = comp_dn[...]

    def put_comp(side, value):
        for c in range(2):
            row = c * (M + 1) + M
            halo[last, side, row : row + 1, :] = value[c : c + 1]

    gather_halo(last, lambda j: cpack_recv[j], put_comp)

    for index, first in enumerate(range(0, M + 1, SUB)):
        halves = ([], [])
        for tile_at in range(WIN + rows - 1 + 2):
            if tile_at < WIN + rows - 1:
                pos = rows - REACH + tile_at
                buffer = outer[pos // rows]
                base = M * 2 * rows + pos % rows
                a = buffer[last, base : base + 1, :]
                b = buffer[last, base + rows : base + rows + 1, :]
            else:
                side = tile_at - (WIN + rows - 1)
                a = halo[last, side, M : M + 1, :]
                b = halo[last, side, 2 * M + 1 : 2 * M + 2, :]
            a = jnp.broadcast_to(a, (SUB, cols))
            b = jnp.broadcast_to(b, (SUB, cols))
            tile = sources(last)[tile_at]
            x, y = tile(0, first), tile(1, first)
            halves[0].append(real_part(a, b, x, y))
            halves[1].append(imag_part(a, b, x, y))
        emit(index, halves, ycbuf, hcbuf)
    windowed(ycbuf, hcbuf, zcbuf)
    comp_count = ycbuf.shape[1]

    def last_field(i, j, p):
        if i > 0:
            return fresh_field(i - 1, j - 1, p)
        other = M if j == 0 else j - 1
        at = (other // SUB) * 2 * SUB + p * SUB + other % SUB
        return zcbuf[pl.ds(at, rows, stride=comp_count), :]

    part[...] = jnp.where(lax.broadcasted_iota(jnp.int32, part.shape, 0) < 1, part[...], 0.0)
    comp_re, comp_im = finish(last, M + 1, last_field)
    comp_out[0] = comp_re
    comp_out[1] = comp_im

    def reduce(count, me, device, source, buffer, sends, recvs):
        copies = []
        for step in range(1, count):
            copy = pltpu.make_async_remote_copy(
                src_ref=source,
                dst_ref=buffer.at[me],
                send_sem=sends.at[step],
                recv_sem=recvs.at[me],
                device_id=device(lax.rem(me + step, count)),
                device_id_type=mesh_id,
            )
            copy.start()
            copies.append(copy)
        buffer[me] = source[...]
        for step in range(1, count):
            other = lax.rem(me + step, count)
            pltpu.make_async_remote_copy(
                src_ref=source,
                dst_ref=buffer.at[other],
                send_sem=sends.at[step],
                recv_sem=recvs.at[other],
                device_id=device(other),
                device_id_type=mesh_id,
            ).wait_recv()
        for copy in copies:
            copy.wait_send()
        total = buffer[0]
        for other in range(1, count):
            total = total + buffer[other]
        return total

    total = reduce(row_count, my_row, lambda d: (d, my_col), part, red_row, send_r, recv_r)
    part2 = red_col.at[col_count]
    part2[...] = total
    total = reduce(col_count, my_col, lambda d: (my_row, d), part2, red_col, send_c, recv_c)
    pixels = rows * cols * row_count * col_count
    for m in range(MS):
        strength[m] = jnp.sum(total[m : m + 1, :]) / pixels

    for m in range(MS):
        each_around(lambda k, m=m: fresh_copy(m, k).wait_send())
    each_around(lambda k: comp_pair(k, True).wait_send())


def shards(slc_stack, land_mask):
    rows, cols = land_mask.shape
    row_count, col_count = lax.axis_size("row"), lax.axis_size("col")
    f32, bf16 = jnp.float32, jnp.bfloat16
    images = (MS, SLOTS * 2 * rows, cols)
    fresh_count = len(FRESH) * 2 * SUB
    comp_count = 2 * SUB * (-(-(M + 1) // SUB))
    vmem = pl.BlockSpec(memory_space=pltpu.VMEM)
    dma = pltpu.SemaphoreType.DMA
    return pl.pallas_call(
        functools.partial(kernel, row_count, col_count),
        out_shape=(
            jax.ShapeDtypeStruct(slc_stack.shape, f32),
            jax.ShapeDtypeStruct((2, rows, cols), f32),
            jax.ShapeDtypeStruct((MS,), f32),
        ),
        in_specs=[vmem, vmem],
        out_specs=(vmem, vmem, pl.BlockSpec(memory_space=pltpu.SMEM)),
        scratch_shapes=[
            pltpu.VMEM(images, f32),
            pltpu.VMEM(images, f32),
            pltpu.VMEM(images, f32),
            pltpu.VMEM((MS, 2, HALO_ROWS, cols), f32),
            pltpu.VMEM((MS, 6, HALO_ROOM, cols), f32),
            pltpu.VMEM((MS, 2, HALO_ROOM, cols), f32),
            pltpu.VMEM((2 * rows, cols), f32),
            pltpu.VMEM((2 * rows, cols), f32),
            pltpu.VMEM((2 * rows, cols), f32),
            pltpu.VMEM((2, SUB, cols), f32),
            pltpu.VMEM((6, SUB, cols), f32),
            pltpu.VMEM((2 * cols, cols), bf16),
            pltpu.VMEM((2 * cols, rows * cols), bf16),
            pltpu.VMEM((rows, fresh_count, 2 * cols), bf16),
            pltpu.VMEM((2, fresh_count, 2 * cols), bf16),
            pltpu.VMEM((rows * fresh_count, cols), f32),
            pltpu.VMEM((rows, comp_count, 2 * cols), bf16),
            pltpu.VMEM((2, comp_count, 2 * cols), bf16),
            pltpu.VMEM((rows * comp_count, cols), f32),
            pltpu.VMEM(((M + 1) * (M + 1), rows, cols), f32),
            pltpu.VMEM((SUB, cols), f32),
            pltpu.VMEM((row_count, SUB, cols), f32),
            pltpu.VMEM((col_count + 1, SUB, cols), f32),
            dma((MS, len(AROUND))),
            dma((MS, len(AROUND))),
            dma((len(AROUND),)),
            dma((len(AROUND),)),
            dma((row_count,)),
            dma((row_count,)),
            dma((col_count,)),
            dma((col_count,)),
        ],
        compiler_params=pltpu.CompilerParams(collective_id=0, has_side_effects=True),
        name="linker",
    )(slc_stack, land_mask)


def solution(mesh):
    return jax.shard_map(
        shards,
        mesh=mesh,
        in_specs=(P(None, None, "row", "col"), P("row", "col")),
        out_specs=(P(None, None, "row", "col"), P(None, "row", "col"), P()),
        check_vma=False,
    )
```

```python
import functools

import jax
import jax.numpy as jnp
from jax import lax
from jax.experimental import pallas as pl
from jax.experimental.pallas import tpu as pltpu
from jax.sharding import PartitionSpec as P

M = 10
MS = 2
WIN = 11
ITERS = 4
REACH = WIN // 2
SUB = 8

covariance_floor = 8.0

AROUND = ((-1, 0), (1, 0), (-1, -1), (0, -1), (1, -1), (-1, 1), (0, 1), (1, 1))
SLOTS = M + SUB
HALO_ROWS = 24
HALO_ROOM = 40


def fresh_units():
    units = [((0, 0, 0), (SUB, 0, 0))]
    for lag in range(1, M):
        for first in range(0, M - lag, SUB):
            units.append(((first, lag, 0), (first, lag, 1)))
    return units


def field_of(units):
    table = {}
    for index, unit in enumerate(units):
        for half, (first, lag, part) in enumerate(unit):
            for lane in range(SUB):
                i = first + lane
                if i + lag < M:
                    table[(i, i + lag, part)] = index * 2 * SUB + half * SUB + lane
    return table


FRESH = fresh_units()
FIELDS = field_of(FRESH)


def window_sums(lines, outputs):
    core = lines[outputs - 1]
    for e in range(outputs, WIN):
        core = core + lines[e]
    low = [None] * outputs
    low[outputs - 1] = core
    for r in range(outputs - 2, -1, -1):
        low[r] = low[r + 1] + lines[r]
    sums = [low[0]]
    high = None
    for r in range(1, outputs):
        extra = lines[WIN - 1 + r]
        high = extra if high is None else high + extra
        sums.append(low[r] + high)
    return sums


def split(value):
    high = value.astype(jnp.bfloat16)
    low = (value - high.astype(jnp.float32)).astype(jnp.bfloat16)
    return high, low


def kernel(
    row_count,
    col_count,
    direct,
    slc_hbm,
    land_hbm,
    linked,
    comp_out,
    strength,
    slc,
    land,
    sig,
    up,
    dn,
    pack_send,
    pack_recv,
    halo,
    comp_send,
    comp_up,
    comp_dn,
    cpack_send,
    cpack_recv,
    w_main,
    w_halo,
    ybuf,
    hbuf,
    zbuf,
    ycbuf,
    hcbuf,
    zcbuf,
    coh,
    part,
    red_row,
    red_col,
    load_sem,
    ready,
    send_a,
    recv_a,
    send_b,
    recv_b,
    send_r,
    recv_r,
    send_c,
    recv_c,
):
    rows, cols = land.shape
    my_row = lax.axis_index("row")
    my_col = lax.axis_index("col")
    strip = rows * REACH
    loads = [
        pltpu.make_async_copy(slc_hbm, slc, load_sem.at[0]),
        pltpu.make_async_copy(land_hbm, land, load_sem.at[1]),
    ]
    for load in loads:
        load.start()

    exists = []
    for dr, dc in AROUND:
        ok = None
        for pos, step, count in ((my_row, dr, row_count), (my_col, dc, col_count)):
            if step:
                here = (pos > 0) if step < 0 else (pos < count - 1)
                ok = here if ok is None else jnp.logical_and(ok, here)
        exists.append(ok)

    for k, (dr, dc) in enumerate(AROUND):

        @pl.when(jnp.logical_not(exists[k]))
        def _(k=k, dc=dc, dr=dr):
            if dc == 0:
                target, small = (up, comp_up) if dr < 0 else (dn, comp_dn)
                for m in range(MS):
                    target[m] = jnp.zeros(target.shape[1:], jnp.float32)
                small[...] = jnp.zeros_like(small)
            else:
                for m in range(MS):
                    pack_recv[m, k - 2] = jnp.zeros(pack_recv.shape[2:], jnp.float32)
                cpack_recv[k - 2] = jnp.zeros(cpack_recv.shape[1:], jnp.float32)

    barrier = pltpu.get_barrier_semaphore()
    mesh_id = pl.DeviceIdType.MESH
    expected = jnp.int32(row_count - 1 + col_count - 1)
    for step in range(1, row_count):
        pl.semaphore_signal(
            barrier, inc=1, device_id=(lax.rem(my_row + step, row_count), my_col), device_id_type=mesh_id
        )
    for step in range(1, col_count):
        pl.semaphore_signal(
            barrier, inc=1, device_id=(my_row, lax.rem(my_col + step, col_count)), device_id_type=mesh_id
        )
    for k, (dr, dc) in enumerate(AROUND):
        if dr and dc:

            @pl.when(exists[k])
            def _(dr=dr, dc=dc):
                pl.semaphore_signal(
                    barrier, inc=1, device_id=(my_row + dr, my_col + dc), device_id_type=mesh_id
                )

            expected = expected + exists[k].astype(jnp.int32)

    for load in loads:
        load.wait()
    mask = land[...].astype(jnp.float32)
    for m in range(MS):
        for i in range(M):
            for c in range(2):
                at = (i * 2 + c) * rows
                sig[m, at : at + rows, :] = slc[m * M + i, c] * mask
        for buffer in (sig, up, dn):
            buffer[m, M * 2 * rows :, :] = jnp.zeros((buffer.shape[1] - M * 2 * rows, cols), jnp.float32)

    lane = lax.broadcasted_iota(jnp.int32, (rows, cols), 1)
    sub = lax.broadcasted_iota(jnp.int32, (rows, cols), 0)
    from_right = (lane >= sub * REACH) & (lane < sub * REACH + REACH)
    from_left = (lane >= (sub + 1) * REACH) & (lane < (sub + 2) * REACH)

    def pack_tile(tile):
        turned = pltpu.roll(tile, REACH, 1, stride=REACH, stride_axis=0)
        high = jnp.sum(jnp.where(from_right, turned, 0.0), axis=0, keepdims=True)
        low = jnp.sum(jnp.where(from_left, turned, 0.0), axis=0, keepdims=True)
        return low, high

    def spread(line, shift):
        total = pltpu.roll(line, cols - shift, 1) if shift else line
        return (
            total
            + pltpu.roll(line, (strip - shift) % cols, 1)
            + pltpu.roll(line, (2 * strip - shift) % cols, 1)
        )

    for m in range(MS):
        pack_send[m] = jnp.zeros(pack_send.shape[1:], jnp.float32)
        for i in range(M):
            for c in range(2):
                low, high = pack_tile(sig[m, (i * 2 + c) * rows : (i * 2 + c + 1) * rows, :])
                pack_send[m, 0, c * (M + 1) + i : c * (M + 1) + i + 1, :] = low
                pack_send[m, 1, c * (M + 1) + i : c * (M + 1) + i + 1, :] = high
        pack_send[m, 0] = spread(pack_send[m, 0], REACH)
        pack_send[m, 1] = spread(pack_send[m, 1], 0)
        pack_recv[m, :, HALO_ROWS:, :] = jnp.zeros((6, HALO_ROOM - HALO_ROWS, cols), jnp.float32)

    pl.semaphore_wait(barrier, expected)

    def mirror(k):
        dr, dc = AROUND[k]
        return AROUND.index((-dr, -dc))

    def fresh_copy(m, k):
        dr, dc = AROUND[k]
        back = mirror(k)
        if dc == 0:
            source = sig.at[m, pl.ds(0, M * 2 * rows)]
            target = (dn if dr < 0 else up).at[m, pl.ds(0, M * 2 * rows)]
        else:
            source = pack_send.at[m, 0 if dc < 0 else 1]
            target = pack_recv.at[m, back - 2, pl.ds(0, HALO_ROWS)]
        return pltpu.make_async_remote_copy(
            src_ref=source,
            dst_ref=target,
            send_sem=send_a.at[m, k],
            recv_sem=recv_a.at[m, back],
            device_id=(my_row + dr, my_col + dc),
            device_id_type=mesh_id,
        )

    def fresh_arrival(m, k):
        dr, dc = AROUND[k]
        if dc == 0:
            source = sig.at[m, pl.ds(0, M * 2 * rows)]
            target = (up if dr < 0 else dn).at[m, pl.ds(0, M * 2 * rows)]
        else:
            source = pack_send.at[m, 0 if dc < 0 else 1]
            target = pack_recv.at[m, k - 2, pl.ds(0, HALO_ROWS)]
        return pltpu.make_async_remote_copy(
            src_ref=source,
            dst_ref=target,
            send_sem=send_a.at[m, k],
            recv_sem=recv_a.at[m, k],
            device_id=(my_row + dr, my_col + dc),
            device_id_type=mesh_id,
        )

    def each_around(action):
        for k in range(len(AROUND)):

            @pl.when(exists[k])
            def _(k=k):
                action(k)

    for m in range(MS):
        each_around(lambda k, m=m: fresh_copy(m, k).start())

    if direct:
        for step in range(1, col_count):
            pl.semaphore_signal(
                ready, inc=1, device_id=(my_row, lax.rem(my_col + step, col_count)), device_id_type=mesh_id
            )

    k_at = lax.broadcasted_iota(jnp.int32, (cols, cols), 0)
    n_at = lax.broadcasted_iota(jnp.int32, (cols, cols), 1)
    near = jnp.where((k_at - n_at <= REACH) & (n_at - k_at <= REACH), 1.0, 0.0).astype(jnp.bfloat16)
    w_main[0:cols, :] = near
    w_main[cols:, :] = near
    line_of = k_at // REACH
    inner = k_at - line_of * REACH
    for side in range(2):
        touches = (n_at <= inner) if side == 0 else (n_at >= inner + cols - REACH)
        line = jnp.where(touches, line_of, -1)
        for r in range(rows):
            first = rows - REACH + r
            w_halo[side * cols : (side + 1) * cols, r * cols : (r + 1) * cols] = jnp.where(
                (line >= first) & (line < first + WIN), 1.0, 0.0
            ).astype(jnp.bfloat16)

    outer = (up, sig, dn)
    lane_halo = lax.broadcasted_iota(jnp.int32, (HALO_ROOM, cols), 1)

    def gather_halo(m, parts, target):
        for side in range(2):
            a, b, c = (parts(side * 3 + j) for j in range(3))
            which = lane_halo[: a.shape[0]]
            target(side, jnp.where(which < strip, a, jnp.where(which < 2 * strip, b, c)))

    def line_tile(m, e, c, first):
        at = rows - REACH + e
        buffer = outer[at // rows]
        return buffer[m, pl.ds((first * 2 + c) * rows + at % rows, SUB, stride=2 * rows), :]

    def halo_tile(m, side, c, first):
        at = c * (M + 1) + first
        return halo[m, side, at : at + SUB, :]

    def emit(index, halves, ytarget, htarget):
        lines_total = WIN + rows - 1
        both = [jnp.concatenate([x, y], 0) for x, y in zip(halves[0], halves[1])]
        at = slice(index * 2 * SUB, (index + 1) * 2 * SUB)
        for r, total in enumerate(window_sums(both[:lines_total], rows)):
            high, low = split(total)
            ytarget[r, at, 0:cols] = high
            ytarget[r, at, cols:] = low
        for side in range(2):
            high, low = split(both[lines_total + side])
            htarget[0, at, side * cols : (side + 1) * cols] = high
            htarget[1, at, side * cols : (side + 1) * cols] = low

    def sources(m):
        lines_total = WIN + rows - 1
        return [functools.partial(line_tile, m, e) for e in range(lines_total)] + [
            functools.partial(halo_tile, m, side) for side in range(2)
        ]

    def real_part(a, b, x, y):
        return a * x + b * y

    def imag_part(a, b, x, y):
        return b * x - a * y

    def fresh_fields(m):
        for index, unit in enumerate(FRESH):
            halves = ([], [])
            for tile in sources(m):
                if index == 0:
                    for half in range(2):
                        first = unit[half][0]
                        a, b = tile(0, first), tile(1, first)
                        halves[half].append(a * a + b * b)
                else:
                    first, lag, _ = unit[0]
                    a, b = tile(0, first), tile(1, first)
                    x, y = tile(0, first + lag), tile(1, first + lag)
                    halves[0].append(real_part(a, b, x, y))
                    halves[1].append(imag_part(a, b, x, y))
            emit(index, halves, ybuf, hbuf)

    def windowed(ysource, hsource, target):
        count = ysource.shape[1]
        main = jnp.dot(
            ysource[...].reshape(rows * count, 2 * cols), w_main[...], preferred_element_type=jnp.float32
        )
        for r in range(rows):
            band = w_halo[:, r * cols : (r + 1) * cols]
            edge = jnp.dot(hsource[0], band, preferred_element_type=jnp.float32) + jnp.dot(
                hsource[1], band, preferred_element_type=jnp.float32
            )
            target[r * count : (r + 1) * count, :] = main[r * count : (r + 1) * count, :] + edge

    fresh_count = len(FRESH) * 2 * SUB

    def fresh_field(i, j, p):
        return zbuf[pl.ds(FIELDS[(i, j, p)], rows, stride=fresh_count), :]

    def power(number, field):
        scales = [
            lax.rsqrt(jnp.maximum(field(i, i, 0), covariance_floor)) for i in range(number)
        ]
        vec_re = [None] * number
        vec_im = [None] * number

        def add(store, i, value):
            store[i] = value if store[i] is None else store[i] + value

        def sub_(store, i, value):
            store[i] = -value if store[i] is None else store[i] - value

        slot = {}
        next_slot = 0
        for i in range(number):
            c = field(i, i, 0) * (scales[i] * scales[i])
            coh[next_slot] = c
            slot[(i, i, 0)] = next_slot
            next_slot += 1
            add(vec_re, i, c)
            for j in range(i + 1, number):
                s = scales[i] * scales[j]
                c = field(i, j, 0) * s
                d = field(i, j, 1) * s
                coh[next_slot] = c
                coh[next_slot + 1] = d
                slot[(i, j, 0)] = next_slot
                slot[(i, j, 1)] = next_slot + 1
                next_slot += 2
                add(vec_re, i, c)
                add(vec_re, j, c)
                add(vec_im, i, d)
                sub_(vec_im, j, d)

        def normalise():
            squares = None
            for i in range(number):
                both = vec_re[i] * vec_re[i] + vec_im[i] * vec_im[i]
                squares = both if squares is None else squares + both
            length = jnp.sqrt(squares)
            inverse = 1.0 / jnp.maximum(length, 1.0)
            return length, [v * inverse for v in vec_re], [v * inverse for v in vec_im]

        length, old_re, old_im = normalise()
        for _ in range(1, ITERS):
            vec_re = [None] * number
            vec_im = [None] * number
            for i in range(number):
                c = coh[slot[(i, i, 0)]]
                add(vec_re, i, c * old_re[i])
                add(vec_im, i, c * old_im[i])
                for j in range(i + 1, number):
                    c = coh[slot[(i, j, 0)]]
                    d = coh[slot[(i, j, 1)]]
                    add(vec_re, i, c * old_re[j] - d * old_im[j])
                    add(vec_im, i, c * old_im[j] + d * old_re[j])
                    add(vec_re, j, c * old_re[i] + d * old_im[i])
                    add(vec_im, j, c * old_im[i] - d * old_re[i])
            length, old_re, old_im = normalise()
        return length, old_re, old_im

    def finish(m, number, field):
        length, re, im = power(number, field)
        re, im = re[number - M :], im[number - M :]
        comp_re = comp_im = None
        for i in range(M):
            a = sig[m, i * 2 * rows : (i * 2 + 1) * rows, :]
            b = sig[m, (i * 2 + 1) * rows : (i * 2 + 2) * rows, :]
            x = re[i] * a + im[i] * b
            y = re[i] * b - im[i] * a
            comp_re = x if comp_re is None else comp_re + x
            comp_im = y if comp_im is None else comp_im + y
            linked[m * M + i, 0] = re[i] * mask
            linked[m * M + i, 1] = im[i] * mask
        share = jnp.sum(mask * length, axis=0, keepdims=True) * (1.0 / number)
        share = share + pltpu.roll(share, cols // 2, 1)
        lane_line = lax.broadcasted_iota(jnp.int32, (1, cols), 1)
        if m == 0:
            part[...] = share
        else:
            part[...] = jnp.where(lane_line < cols // 2, part[...], share)
        return comp_re, comp_im

    def take_fresh(m):
        each_around(lambda k: fresh_arrival(m, k).wait_recv())

        def put(side, value):
            halo[m, side] = value

        gather_halo(m, lambda j: pack_recv[m, j], put)

    take_fresh(0)
    fresh_fields(0)
    windowed(ybuf, hbuf, zbuf)
    comp_re, comp_im = finish(0, M, fresh_field)
    comp_send[0:rows, :] = comp_re
    comp_send[rows:, :] = comp_im
    cpack_send[...] = jnp.zeros_like(cpack_send)
    for c, value in enumerate((comp_re, comp_im)):
        low, high = pack_tile(value)
        cpack_send[0, c : c + 1, :] = spread(low, REACH)
        cpack_send[1, c : c + 1, :] = spread(high, 0)

    def comp_pair(k, sending):
        dr, dc = AROUND[k]
        slot = mirror(k) if sending else k
        if dc == 0:
            source = comp_send
            target = comp_up if AROUND[slot][0] < 0 else comp_dn
        else:
            source = cpack_send.at[0 if dc < 0 else 1]
            target = cpack_recv.at[slot - 2]
        return pltpu.make_async_remote_copy(
            src_ref=source,
            dst_ref=target,
            send_sem=send_b.at[k],
            recv_sem=recv_b.at[slot],
            device_id=(my_row + dr, my_col + dc),
            device_id_type=mesh_id,
        )

    each_around(lambda k: comp_pair(k, True).start())

    last = MS - 1
    take_fresh(last)
    fresh_fields(last)
    windowed(ybuf, hbuf, zbuf)

    each_around(lambda k: comp_pair(k, False).wait_recv())
    at = M * 2 * rows
    sig[last, at : at + 2 * rows, :] = comp_send[...]
    up[last, at : at + 2 * rows, :] = comp_up[...]
    dn[last, at : at + 2 * rows, :] = comp_dn[...]

    def put_comp(side, value):
        for c in range(2):
            row = c * (M + 1) + M
            halo[last, side, row : row + 1, :] = value[c : c + 1]

    gather_halo(last, lambda j: cpack_recv[j], put_comp)

    for index, first in enumerate(range(0, M + 1, SUB)):
        halves = ([], [])
        for tile_at in range(WIN + rows - 1 + 2):
            if tile_at < WIN + rows - 1:
                pos = rows - REACH + tile_at
                buffer = outer[pos // rows]
                base = M * 2 * rows + pos % rows
                a = buffer[last, base : base + 1, :]
                b = buffer[last, base + rows : base + rows + 1, :]
            else:
                side = tile_at - (WIN + rows - 1)
                a = halo[last, side, M : M + 1, :]
                b = halo[last, side, 2 * M + 1 : 2 * M + 2, :]
            a = jnp.broadcast_to(a, (SUB, cols))
            b = jnp.broadcast_to(b, (SUB, cols))
            tile = sources(last)[tile_at]
            x, y = tile(0, first), tile(1, first)
            halves[0].append(real_part(a, b, x, y))
            halves[1].append(imag_part(a, b, x, y))
        emit(index, halves, ycbuf, hcbuf)
    windowed(ycbuf, hcbuf, zcbuf)
    comp_count = ycbuf.shape[1]

    def last_field(i, j, p):
        if i > 0:
            return fresh_field(i - 1, j - 1, p)
        other = M if j == 0 else j - 1
        at = (other // SUB) * 2 * SUB + p * SUB + other % SUB
        return zcbuf[pl.ds(at, rows, stride=comp_count), :]

    comp_re, comp_im = finish(last, M + 1, last_field)
    comp_out[0] = comp_re
    comp_out[1] = comp_im

    def reduce(count, me, device, source, buffer, sends, recvs):
        copies = []
        for step in range(1, count):
            copy = pltpu.make_async_remote_copy(
                src_ref=source,
                dst_ref=buffer.at[me],
                send_sem=sends.at[step],
                recv_sem=recvs.at[me],
                device_id=device(lax.rem(me + step, count)),
                device_id_type=mesh_id,
            )
            copy.start()
            copies.append(copy)
        buffer[me] = source[...]
        for step in range(1, count):
            other = lax.rem(me + step, count)
            pltpu.make_async_remote_copy(
                src_ref=source,
                dst_ref=buffer.at[other],
                send_sem=sends.at[step],
                recv_sem=recvs.at[other],
                device_id=device(other),
                device_id_type=mesh_id,
            ).wait_recv()
        for copy in copies:
            copy.wait_send()
        total = buffer[0]
        for other in range(1, count):
            total = total + buffer[other]
        return total

    if direct:
        pl.semaphore_wait(ready, col_count - 1)
        me = my_row * col_count + my_col
        total = reduce(
            row_count * col_count, me, lambda d: (d // col_count, d % col_count), part, red_row, send_r, recv_r
        )
    else:
        total = reduce(row_count, my_row, lambda d: (d, my_col), part, red_row, send_r, recv_r)
        part2 = red_col.at[col_count]
        part2[...] = total
        total = reduce(col_count, my_col, lambda d: (my_row, d), part2, red_col, send_c, recv_c)
    strength[...] = total

    for m in range(MS):
        each_around(lambda k, m=m: fresh_copy(m, k).wait_send())
    each_around(lambda k: comp_pair(k, True).wait_send())


def closing(pixels, linked_in, comp_in, total, linked, comp, strength, sems):
    copies = [
        pltpu.make_async_copy(linked_in, linked, sems.at[0]),
        pltpu.make_async_copy(comp_in, comp, sems.at[1]),
    ]
    for copy in copies:
        copy.start()
    for m in range(MS):
        lane = lax.broadcasted_iota(jnp.int32, total.shape, 1)
        mine = lane < total.shape[1] // 2 if m == 0 else lane >= total.shape[1] // 2
        strength[m] = jnp.sum(jnp.where(mine, total[...], 0.0)) / pixels
    for copy in copies:
        copy.wait()


def shards(slc_stack, land_mask):
    rows, cols = land_mask.shape
    row_count, col_count = lax.axis_size("row"), lax.axis_size("col")
    f32, bf16 = jnp.float32, jnp.bfloat16
    images = (MS, SLOTS * 2 * rows, cols)
    fresh_count = len(FRESH) * 2 * SUB
    comp_count = 2 * SUB * (-(-(M + 1) // SUB))
    vmem = pl.BlockSpec(memory_space=pltpu.VMEM)
    dma = pltpu.SemaphoreType.DMA
    hbm = pl.BlockSpec(memory_space=pltpu.HBM)
    devices = row_count * col_count
    direct = devices <= 64
    peers = devices if direct else row_count
    linked_shape = jax.ShapeDtypeStruct(slc_stack.shape, f32)
    comp_shape = jax.ShapeDtypeStruct((2, rows, cols), f32)
    linked, comp, total = pl.pallas_call(
        functools.partial(kernel, row_count, col_count, direct),
        out_shape=(linked_shape, comp_shape, jax.ShapeDtypeStruct((1, cols), f32)),
        in_specs=[hbm, hbm],
        out_specs=(vmem, vmem, vmem),
        scratch_shapes=[
            pltpu.VMEM(slc_stack.shape, f32),
            pltpu.VMEM((rows, cols), jnp.int32),
            pltpu.VMEM(images, f32),
            pltpu.VMEM(images, f32),
            pltpu.VMEM(images, f32),
            pltpu.VMEM((MS, 2, HALO_ROWS, cols), f32),
            pltpu.VMEM((MS, 6, HALO_ROOM, cols), f32),
            pltpu.VMEM((MS, 2, HALO_ROOM, cols), f32),
            pltpu.VMEM((2 * rows, cols), f32),
            pltpu.VMEM((2 * rows, cols), f32),
            pltpu.VMEM((2 * rows, cols), f32),
            pltpu.VMEM((2, SUB, cols), f32),
            pltpu.VMEM((6, SUB, cols), f32),
            pltpu.VMEM((2 * cols, cols), bf16),
            pltpu.VMEM((2 * cols, rows * cols), bf16),
            pltpu.VMEM((rows, fresh_count, 2 * cols), bf16),
            pltpu.VMEM((2, fresh_count, 2 * cols), bf16),
            pltpu.VMEM((rows * fresh_count, cols), f32),
            pltpu.VMEM((rows, comp_count, 2 * cols), bf16),
            pltpu.VMEM((2, comp_count, 2 * cols), bf16),
            pltpu.VMEM((rows * comp_count, cols), f32),
            pltpu.VMEM(((M + 1) * (M + 1), rows, cols), f32),
            pltpu.VMEM((1, cols), f32),
            pltpu.VMEM((peers, 1, cols), f32),
            pltpu.VMEM((col_count + 1, 1, cols), f32),
            dma((2,)),
            pltpu.SemaphoreType.REGULAR,
            dma((MS, len(AROUND))),
            dma((MS, len(AROUND))),
            dma((len(AROUND),)),
            dma((len(AROUND),)),
            dma((peers,)),
            dma((peers,)),
            dma((col_count,)),
            dma((col_count,)),
        ],
        compiler_params=pltpu.CompilerParams(collective_id=0, has_side_effects=True, vmem_limit_bytes=16 << 20),
        name="linker",
    )(*(pltpu.with_memory_space_constraint(x, pltpu.HBM) for x in (slc_stack, land_mask)))
    return pl.pallas_call(
        functools.partial(closing, rows * cols * devices),
        out_shape=(linked_shape, comp_shape, jax.ShapeDtypeStruct((MS,), f32)),
        in_specs=[vmem, vmem, vmem],
        out_specs=(hbm, hbm, pl.BlockSpec(memory_space=pltpu.SMEM)),
        scratch_shapes=[dma((2,))],
        compiler_params=pltpu.CompilerParams(vmem_limit_bytes=4 << 20),
        name="closing",
    )(linked, comp, total)


def solution(mesh):
    return jax.shard_map(
        shards,
        mesh=mesh,
        in_specs=(P(None, None, "row", "col"), P("row", "col")),
        out_specs=(P(None, None, "row", "col"), P(None, "row", "col"), P()),
        check_vma=False,
    )
```
